128 devices in a mesh: layer: 8 (over z_lo, y), lat: 16 (over x, z_hi, core).
Axes of the slice: x: 4, y: 4, z: 4 (z_hi: 2, z_lo: 2; z = z_hi * 2 + z_lo), core: 2. Of those that a mesh axis runs over, the one named last changes fastest.
Arguments:
- activations: bfloat16 [8, 512, 2048], P(None, None, 'layer'), may hold values from -6 to 6
- targets: bfloat16 [8, 512, 2048], P(None, None, 'layer'), may hold values from -6 to 6
- encoder: bfloat16 [8, 2048, 8192], P(None, 'layer', 'lat'), may hold values from -0.125 to 0.125
- bias: float32 [8, 8192], P(None, 'lat'), may hold values from -3 to 3
- decoder: bfloat16 [36, 8192, 2048], P(None, 'lat', 'layer'), may hold values from -0.75 to 0.75
- active: int32 [8, 512, 64], replicated, may hold values from 0 to 8191, all different within a row
Outputs:
- grad_encoder: bfloat16 [8, 2048, 8192], P(None, 'layer', 'lat')
- grad_bias: float32 [8, 8192], P(None, 'lat')
- grad_decoder: bfloat16 [36, 8192, 2048], P(None, 'lat', 'layer')
The draws below stay inside these ranges and needn't reach their ends.
Inputs may be any that keep to these rules, and one draw needn't show every extreme that they name: `active`: each row names 64 different latents.
All inputs are finite; a program needn't handle non-finite values.
Results may differ from the reference program's by a relative error of at most 0.0064.
Values may be sent and summed in bfloat16 or wider, within the bound.
No kernel may reach another device: no remote copies, remote signals or barrier semaphores. Data moves between devices by JAX's collectives and lax.ppermute only.
A program may use at most 128 MiB of HBM per device.

```python
import jax
import jax.numpy as jnp
from jax import lax

D = 2048
F = 8192
K = 64
LAYERS = 8
TOKENS = 512
PAIRS = 36


def shard_levels(key, dims, cuts, least, largest):
    def one(axis_at, parts):
        draws = jax.random.uniform(jax.random.fold_in(jax.random.fold_in(key, 6), axis_at), (parts,), jnp.float32, least / len(cuts), largest / len(cuts))
        return jnp.repeat(jnp.exp(draws), dims[axis_at] // parts).reshape((-1,) + (1,) * (len(dims) - axis_at - 1))

    gain = one(*cuts[0])
    for cut in cuts[1:]:
        gain = gain * one(*cut)
    return gain


def picks_of(rng, rows, count, top, lift):
    order = jax.random.permutation(jax.random.fold_in(rng, 1), count)
    favour = order
    for power in range(3):
        favour = favour * favour // count
    favour = favour * lift // count
    lots = jax.random.randint(jax.random.fold_in(rng, 2), (rows, count), 0, 4096) + favour
    sure = jax.random.permutation(jax.random.fold_in(rng, 3), rows)[jnp.arange(count) % rows]
    lots = jnp.where(jnp.arange(rows)[:, None] == sure[None, :], 1 << 14, lots)
    merit = lots * count + jnp.arange(count)
    return lax.top_k(merit.astype(jnp.int32), top)[1].astype(jnp.int32)


def bell_draw(key, shape, deviation, bound, shards=(), held_as=jnp.bfloat16):
    loudness = shard_levels(key, shape, shards, -0.22, 0.18) if shards else 1.0
    array = jax.random.normal(key, shape, jnp.float32) * deviation * loudness
    return jnp.minimum(jnp.maximum(array, -bound), bound).astype(held_as)


def setup_inputs(seed: int = 0) -> dict:
    seeds = jax.random.split(jax.random.key(seed), 7)
    activations = bell_draw(seeds[0], (LAYERS, TOKENS, D), 1.0, 6.0, ((2, 8),))
    targets = bell_draw(seeds[1], (LAYERS, TOKENS, D), 1.0, 6.0, ((2, 8),))
    encoder = bell_draw(seeds[2], (LAYERS, D, F), D ** -0.5, 0.125, ((1, 8), (2, 16)))
    bias = bell_draw(seeds[3], (LAYERS, F), 0.5, 3.0, ((1, 16),), jnp.float32)
    decoder = bell_draw(seeds[4], (PAIRS, F, D), K ** -0.5, 0.75, ((1, 16), (2, 8)))
    active = picks_of(seeds[5], LAYERS * TOKENS, F, K, 128).reshape((LAYERS, TOKENS, K))
    return {"activations": activations, "targets": targets, "encoder": encoder, "bias": bias, "decoder": decoder, "active": active}


def pair_index(source, target):
    return source * LAYERS - source * (source - 1) // 2 + (target - source)


def reference(activations, targets, encoder, bias, decoder, active):
    token_ids = jnp.arange(TOKENS, dtype=jnp.int32)
    masks = []
    latent_act = []
    for source in range(LAYERS):
        layer_mask = jnp.zeros((TOKENS, F), jnp.float32).at[token_ids[:, None], active[source]].set(1.0)
        preact = jnp.dot(activations[source], encoder[source], preferred_element_type=jnp.float32) + bias[source][None, :]
        masks.append(layer_mask)
        latent_act.append((preact * layer_mask).astype(jnp.bfloat16))
    errors = []
    for target in range(LAYERS):
        rebuilt = jnp.zeros((TOKENS, D), jnp.float32)
        for source in range(target + 1):
            rebuilt = rebuilt + jnp.dot(latent_act[source], decoder[pair_index(source, target)], preferred_element_type=jnp.float32)
        errors.append((rebuilt - targets[target].astype(jnp.float32)).astype(jnp.bfloat16))
    grad_decoder = []
    for source in range(LAYERS):
        for target in range(source, LAYERS):
            grad_decoder.append(jnp.dot(latent_act[source].T, errors[target], preferred_element_type=jnp.float32).astype(jnp.bfloat16))
    grad_encoder = []
    grad_bias = []
    for source in range(LAYERS):
        grad_act = jnp.zeros((TOKENS, F), jnp.float32)
        for target in range(source, LAYERS):
            grad_act = grad_act + jnp.dot(errors[target], decoder[pair_index(source, target)].T, preferred_element_type=jnp.float32)
        grad_pre = (grad_act * masks[source]).astype(jnp.bfloat16)
        grad_encoder.append(jnp.dot(activations[source].T, grad_pre, preferred_element_type=jnp.float32).astype(jnp.bfloat16))
        grad_bias.append(jnp.sum(grad_pre.astype(jnp.float32), axis=0))
    return jnp.stack(grad_encoder), jnp.stack(grad_bias), jnp.stack(grad_decoder)
```

```python
import jax
import jax.numpy as jnp
from jax import lax
from jax.experimental import pallas as pl
from jax.experimental.pallas import tpu as pltpu
from jax.sharding import PartitionSpec as P

LAYERS = 8
T = 512
HALF = T // 2
DW = 256
FW = 512
PAIRS = LAYERS * (LAYERS + 1) // 2
BF = jnp.bfloat16
F32 = jnp.float32
I32 = jnp.int32
BIG = pltpu.CompilerParams(
    dimension_semantics=("arbitrary",), vmem_limit_bytes=60 * 1024 * 1024
)


def first_pair(source):
    return source * LAYERS - source * (source - 1) // 2


def take(x, index):
    return jnp.take_along_axis(x, index, axis=1)


def lanes(rows):
    return lax.broadcasted_iota(I32, (rows, 128), 1)


def slot_columns(table):
    lane = lanes(table.shape[0])
    base = lane & 64
    r = lane & 63
    word_at = jnp.zeros_like(r)
    before = jnp.zeros_like(r)
    for step in (8, 4, 2, 1):
        tried = word_at + step
        count = take(table, base + 16 + tried)
        good = count <= r
        word_at = jnp.where(good, tried, word_at)
        before = jnp.where(good, count, before)
    left = take(table, base + word_at)
    k = r - before
    spot = jnp.zeros_like(r)
    for step in (16, 8, 4, 2, 1):
        low = lax.population_count(left & ((1 << step) - 1))
        good = k >= low
        k = jnp.where(good, k - low, k)
        left = jnp.where(good, lax.shift_right_logical(left, jnp.full_like(left, step)), left)
        spot = jnp.where(good, spot + step, spot)
    return word_at * 32 + spot


def pack(read, columns):
    lane = lanes(HALF)
    within = columns & 127
    chunk_of = lax.shift_right_logical(columns, jnp.full_like(columns, 7))
    packed = None
    for chunk in range(FW // 128):
        picked = jnp.where(
            lane < 64, take(read(0, chunk), within), take(read(1, chunk), within)
        )
        packed = picked if packed is None else jnp.where(chunk_of == chunk, picked, packed)
    return packed


def unpack(table, slots, write):
    lane = lanes(HALF)
    bit = lane & 31
    below = lax.shift_left(jnp.full_like(bit, 1), bit) - 1
    for half in range(2):
        for chunk in range(FW // 128):
            at = 64 * half + 4 * chunk + lax.shift_right_logical(lane, jnp.full_like(lane, 5))
            word = take(table, at)
            before = take(table, at + 16)
            rank = before + lax.population_count(word & below)
            value = take(slots, (rank + 64 * half) & 127)
            hit = (lax.shift_right_logical(word, bit) & 1) == 1
            write(half, chunk, jnp.where(hit, value, 0.0))


def encode_kernel(info, active, acts, encoder, bias, table_out, columns_out, slots_out, rows, dense):
    first = info[0]
    rel = active[0] - first
    high = lax.shift_right_arithmetic(rel, jnp.full_like(rel, 5))
    bits = lax.shift_left(jnp.full_like(rel, 1), rel & 31)
    rows[...] = jnp.zeros_like(rows)
    before = jnp.zeros((1, T), I32)
    for word in range(16):
        marked = jnp.where(high == word, bits, 0)
        folded = marked[0:8]
        for k in range(8, 64, 8):
            folded = folded | marked[k : k + 8]
        whole = jnp.sum(folded, axis=0, keepdims=True)
        for half in range(2):
            part = slice(half * HALF, (half + 1) * HALF)
            rows[64 * half + word : 64 * half + word + 1, :] = whole[:, part]
            rows[64 * half + 16 + word : 64 * half + 17 + word, :] = before[:, part]
        before = before + lax.population_count(whole)
    table = rows[...].T
    table_out[0] = table
    columns = slot_columns(table)
    columns_out[0] = columns
    value = jnp.dot(acts[0], encoder[0], preferred_element_type=F32)
    dense[...] = value + bias[0] * info[1].astype(F32)
    slots_out[0] = pack(
        lambda half, chunk: dense[pl.ds(half * HALF, HALF), pl.ds(chunk * 128, 128)], columns
    ).astype(BF)


def one(*shape):
    return pl.BlockSpec((1,) + shape, lambda i, *_: (i,) + (0,) * len(shape))


def whole(*shape):
    return pl.BlockSpec(shape, lambda i, *_: (0,) * len(shape))


ANY = pl.BlockSpec(memory_space=pl.ANY)


def encode(info, active_t, activations, encoder, bias):
    return pl.pallas_call(
        encode_kernel,
        grid_spec=pltpu.PrefetchScalarGridSpec(
            num_scalar_prefetch=1,
            grid=(LAYERS,),
            in_specs=[one(64, T), one(T, DW), one(DW, FW), one(1, FW)],
            out_specs=[one(HALF, 128), one(HALF, 128), one(HALF, 128)],
            scratch_shapes=[pltpu.VMEM((128, HALF), I32), pltpu.VMEM((T, FW), F32)],
        ),
        out_shape=[
            jax.ShapeDtypeStruct((LAYERS, HALF, 128), I32),
            jax.ShapeDtypeStruct((LAYERS, HALF, 128), I32),
            jax.ShapeDtypeStruct((LAYERS, HALF, 128), BF),
        ],
        compiler_params=BIG,
        name="encode",
    )(info, active_t, activations, encoder, bias[:, None, :])


def load_decoder(decoder, held, arrived):
    @pl.when(pl.program_id(0) == 0)
    def _():
        @pl.loop(0, PAIRS)
        def _(p):
            pltpu.make_async_copy(decoder.at[p], held.at[p], arrived.at[p]).start()


def rebuild_kernel(info, table, slots, decoder, latent_out, own_out, send_out, total, held, arrived):
    source = pl.program_id(0)
    load_decoder(decoder, held, arrived)

    @pl.when(source == 0)
    def _():
        total[...] = jnp.zeros_like(total)

    def write(half, chunk, part):
        latent_out[0, pl.ds(half * HALF, HALF), pl.ds(chunk * 128, 128)] = part.astype(BF)

    unpack(table[0], slots[0].astype(F32), write)

    @pl.loop(source, LAYERS)
    def _(target):
        p = first_pair(source) + target - source
        pltpu.make_async_copy(decoder.at[p], held.at[p], arrived.at[p]).wait()
        total[target] += jnp.dot(latent_out[0], held[p], preferred_element_type=F32)

    @pl.when(source == LAYERS - 1)
    def _():
        core = info[2]
        for i in range(LAYERS // 2):
            own_out[i] = total[core * 4 + i]
            send_out[i] = total[(1 - core) * 4 + i].astype(BF)


def rebuild(info, table, slots, decoder):
    return pl.pallas_call(
        rebuild_kernel,
        grid_spec=pltpu.PrefetchScalarGridSpec(
            num_scalar_prefetch=1,
            grid=(LAYERS,),
            in_specs=[one(HALF, 128), one(HALF, 128), ANY],
            out_specs=[one(T, FW), whole(4, T, DW), whole(4, T, DW)],
            scratch_shapes=[
                pltpu.VMEM((LAYERS, T, DW), F32),
                pltpu.VMEM((PAIRS, FW, DW), BF),
                pltpu.SemaphoreType.DMA((PAIRS,)),
            ],
        ),
        out_shape=[
            jax.ShapeDtypeStruct((LAYERS, T, FW), BF),
            jax.ShapeDtypeStruct((4, T, DW), F32),
            jax.ShapeDtypeStruct((4, T, DW), BF),
        ],
        compiler_params=BIG,
        name="rebuild",
    )(info, table, slots, decoder)


def grad_act_kernel(columns, errors, decoder, slots_out, total, held, arrived):
    source = pl.program_id(0)
    load_decoder(decoder, held, arrived)
    total[...] = jnp.zeros_like(total)

    @pl.loop(source, LAYERS)
    def _(target):
        p = first_pair(source) + target - source
        pltpu.make_async_copy(decoder.at[p], held.at[p], arrived.at[p]).wait()
        total[...] += lax.dot_general(
            errors[target], held[p], (((1,), (1,)), ((), ())), preferred_element_type=F32
        )

    slots_out[0] = pack(
        lambda half, chunk: total[pl.ds(half * HALF, HALF), pl.ds(chunk * 128, 128)], columns[0]
    ).astype(BF)


def grad_act(columns, errors, decoder):
    return pl.pallas_call(
        grad_act_kernel,
        grid=(LAYERS,),
        in_specs=[one(HALF, 128), whole(LAYERS, T, DW), ANY],
        out_specs=one(HALF, 128),
        out_shape=jax.ShapeDtypeStruct((LAYERS, HALF, 128), BF),
        scratch_shapes=[
            pltpu.VMEM((T, FW), F32),
            pltpu.VMEM((PAIRS, FW, DW), BF),
            pltpu.SemaphoreType.DMA((PAIRS,)),
        ],
        compiler_params=BIG,
        name="grad_act",
    )(columns, errors, decoder)


def grad_decoder_kernel(latent, errors, grad_out, turned, held, sent):
    source = pl.program_id(0)
    turned[...] = latent[0].T

    @pl.loop(source, LAYERS)
    def _(target):
        p = first_pair(source) + target - source
        held[p] = jnp.dot(turned[...], errors[target], preferred_element_type=F32).astype(BF)
        pltpu.make_async_copy(held.at[p], grad_out.at[p], sent.at[p]).start()

    @pl.when(source == LAYERS - 1)
    def _():
        @pl.loop(0, PAIRS)
        def _(p):
            pltpu.make_async_copy(held.at[p], grad_out.at[p], sent.at[p]).wait()


def grad_decoder_of(latent, errors):
    return pl.pallas_call(
        grad_decoder_kernel,
        grid=(LAYERS,),
        in_specs=[one(T, FW), whole(LAYERS, T, DW)],
        out_specs=ANY,
        out_shape=jax.ShapeDtypeStruct((PAIRS, FW, DW), BF),
        scratch_shapes=[
            pltpu.VMEM((FW, T), BF),
            pltpu.VMEM((PAIRS, FW, DW), BF),
            pltpu.SemaphoreType.DMA((PAIRS,)),
        ],
        compiler_params=BIG,
        name="grad_decoder",
    )(latent, errors)


def grad_encoder_kernel(table, slots, acts, grad_out, bias_out, dense):
    def write(half, chunk, part):
        dense[pl.ds(half * HALF, HALF), pl.ds(chunk * 128, 128)] = part.astype(BF)

    unpack(table[0], slots[0].astype(F32), write)
    grad = dense[...]
    grad_out[0] = lax.dot_general(
        acts[0], grad, (((0,), (0,)), ((), ())), preferred_element_type=F32
    ).astype(BF)
    bias_out[0] = jnp.sum(grad.astype(F32), axis=0, keepdims=True)


def grad_encoder_of(table, slots, activations):
    grad, bias = pl.pallas_call(
        grad_encoder_kernel,
        grid=(LAYERS,),
        in_specs=[one(HALF, 128), one(HALF, 128), one(T, DW)],
        out_specs=[one(DW, FW), one(1, FW)],
        out_shape=[
            jax.ShapeDtypeStruct((LAYERS, DW, FW), BF),
            jax.ShapeDtypeStruct((LAYERS, 1, FW), F32),
        ],
        scratch_shapes=[pltpu.VMEM((T, FW), BF)],
        compiler_params=BIG,
        name="grad_encoder",
    )(table, slots, activations)
    return grad, bias[:, 0, :]


CHIPS = [[2 * chip + core for chip in range(8)] for core in range(2)]


def swap_cores(x):
    return lax.ppermute(x, "lat", [(i, i ^ 1) for i in range(16)])


def over_layer(x):
    return lax.all_to_all(x, "layer", 0, 0, tiled=True)


def over_chips(x):
    return lax.all_to_all(x, "lat", 0, 0, axis_index_groups=CHIPS, tiled=True)


def sum_slots(slots):
    own = jnp.sum(over_layer(slots).astype(F32), axis=0).astype(BF)
    return over_layer(jnp.broadcast_to(own[None], slots.shape))


def on_device(activations, targets, encoder, bias, decoder, active):
    lat = lax.axis_index("lat")
    core = lat % 2
    info = jnp.stack(
        [lat * FW, (lax.axis_index("layer") == 0).astype(I32), core]
    ).astype(I32)
    table, columns, partial = encode(info, jnp.swapaxes(active, 1, 2), activations, encoder, bias)
    latent_slots = sum_slots(partial)
    latent, own, send = rebuild(info, table, latent_slots, decoder)
    half = (own + swap_cores(send).astype(F32)).astype(BF).reshape(8, 256, DW)
    mine = jnp.sum(over_chips(half).astype(F32), axis=0)
    first_row = (core * 8 + lat // 2) * 256
    wanted = lax.dynamic_slice_in_dim(targets.reshape(LAYERS * T, DW), first_row, 256)
    error = (mine - wanted.astype(F32)).astype(BF)
    error_half = over_chips(jnp.broadcast_to(error[None], (8, 256, DW)))
    other_half = swap_cores(error_half)
    low = jnp.where(core == 0, error_half, other_half)
    high = jnp.where(core == 0, other_half, error_half)
    errors = jnp.concatenate([low, high]).reshape(LAYERS, T, DW)
    grad_slots = sum_slots(grad_act(columns, errors, decoder))
    grad_decoder = grad_decoder_of(latent, errors)
    grad_encoder, grad_bias = grad_encoder_of(table, grad_slots, activations)
    return (grad_encoder, grad_bias, grad_decoder)


def solution(mesh):
    placed = (
        P(None, None, "layer"),
        P(None, None, "layer"),
        P(None, "layer", "lat"),
        P(None, "lat"),
        P(None, "lat", "layer"),
        P(),
    )
    return jax.shard_map(
        on_device,
        mesh=mesh,
        in_specs=placed,
        out_specs=(P(None, "layer", "lat"), P(None, "lat"), P(None, "lat", "layer")),
        check_vma=False,
    )
```

```python
import jax
import jax.numpy as jnp
from jax import lax
from jax.experimental import pallas as pl
from jax.experimental.pallas import tpu as pltpu
from jax.sharding import PartitionSpec as P

LAYERS = 8
T = 512
HALF = T // 2
DW = 256
FW = 512
ROWS = 256
PAIRS = LAYERS * (LAYERS + 1) // 2
BF = jnp.bfloat16
F32 = jnp.float32
I32 = jnp.int32
ANY = pl.BlockSpec(memory_space=pl.ANY)
HELD = pl.BlockSpec(memory_space=pltpu.VMEM)


def params(steps=0):
    return pltpu.CompilerParams(
        dimension_semantics=("arbitrary",) * steps, vmem_limit_bytes=60 * 1024 * 1024
    )


def first_pair(source):
    return source * LAYERS - source * (source - 1) // 2


def take(x, index):
    return jnp.take_along_axis(x, index, axis=1)


def lanes(rows):
    return lax.broadcasted_iota(I32, (rows, 128), 1)


def right(x, by):
    return lax.shift_right_logical(x, jnp.full_like(x, by) if isinstance(by, int) else by)


def slot_columns(table):
    lane = lanes(table.shape[0])
    base = lane & 64
    r = lane & 63
    at = jnp.zeros_like(r)
    entry = take(table, base)
    for step in (16, 8, 4, 2, 1):
        found = take(table, base + at + step)
        good = right(found, 16) <= r
        at = jnp.where(good, at + step, at)
        entry = jnp.where(good, found, entry)
    k = r - right(entry, 16)
    left = entry & 0xFFFF
    spot = jnp.zeros_like(r)
    for step in (8, 4, 2, 1):
        low = lax.population_count(left & ((1 << step) - 1))
        good = k >= low
        k = jnp.where(good, k - low, k)
        left = jnp.where(good, right(left, step), left)
        spot = jnp.where(good, spot + step, spot)
    return at * 16 + spot


def pack(dense, columns_at, write):
    lane = lanes(ROWS)

    @pl.loop(0, HALF // ROWS)
    def _(block):
        row = pl.multiple_of(block * ROWS, ROWS)
        columns = columns_at(row)
        within = columns & 127
        chunk_of = right(columns, 7)
        packed = None
        for chunk in range(FW // 128):
            part = pl.ds(chunk * 128, 128)
            low = take(dense[pl.ds(row, ROWS), part], within)
            high = take(dense[pl.ds(row + HALF, ROWS), part], within)
            picked = jnp.where(lane < 64, low, high)
            packed = picked if packed is None else jnp.where(chunk_of == chunk, picked, packed)
        write(row, packed.astype(BF))


def unpack(ranks, slots, dense):
    @pl.loop(0, HALF // ROWS)
    def _(block):
        row = pl.multiple_of(block * ROWS, ROWS)
        values = slots[pl.ds(row, ROWS), :].astype(F32)
        for half in range(2):
            for chunk in range(FW // 128):
                place = (pl.ds(row + half * HALF, ROWS), pl.ds(chunk * 128, 128))
                rank = ranks[place]
                value = jnp.where(rank >= 0, take(values, rank & 127), 0.0)
                dense[place] = value.astype(BF)


def encode_kernel(active, acts, encoder, bias, table_out, columns_out, slots_out, rows, dense):
    layer = pl.program_id(0)
    rel = active[0] - lax.axis_index("lat") * FW
    high = lax.shift_right_arithmetic(rel, jnp.full_like(rel, 5))
    bits = lax.shift_left(jnp.full_like(rel, 1), rel & 31)

    @pl.when(layer == 0)
    def _():
        rows[...] = jnp.zeros_like(rows)

    before = jnp.zeros((1, T), I32)
    for word in range(16):
        marked = jnp.where(high == word, bits, 0)
        folded = marked[0:8]
        for k in range(8, 64, 8):
            folded = folded | marked[k : k + 8]
        both = jnp.sum(folded, axis=0, keepdims=True)
        for part in range(2):
            piece = both & 0xFFFF if part == 0 else right(both, 16)
            entry = piece | lax.shift_left(before, jnp.full_like(before, 16))
            before = before + lax.population_count(piece)
            for half in range(2):
                at = 64 * half + 2 * word + part
                rows[at : at + 1, :] = entry[:, half * HALF : (half + 1) * HALF]
    table_out[0] = rows[...].T

    @pl.loop(0, HALF // ROWS)
    def _(block):
        at = (0, pl.ds(pl.multiple_of(block * ROWS, ROWS), ROWS), slice(None))
        columns_out[at] = slot_columns(table_out[at])

    added = jnp.where(lax.axis_index("layer") == 0, 1.0, 0.0).astype(F32)
    value = jnp.dot(acts[0], encoder[0], preferred_element_type=F32)
    dense[...] = value + bias[pl.ds(layer, 1), :] * added

    def write(row, packed):
        slots_out[0, pl.ds(row, ROWS), :] = packed

    pack(dense, lambda row: columns_out[0, pl.ds(row, ROWS), :], write)


def one(*shape):
    return pl.BlockSpec((1,) + shape, lambda i: (i,) + (0,) * len(shape))


def whole(*shape):
    return pl.BlockSpec(shape, lambda i: (0,) * len(shape))


def encode(active_t, activations, encoder, bias):
    return pl.pallas_call(
        encode_kernel,
        grid=(LAYERS,),
        in_specs=[one(64, T), one(T, DW), one(DW, FW), whole(LAYERS, FW)],
        out_specs=[one(HALF, 128), one(HALF, 128), one(HALF, 128)],
        out_shape=[
            jax.ShapeDtypeStruct((LAYERS, HALF, 128), I32),
            jax.ShapeDtypeStruct((LAYERS, HALF, 128), I32),
            jax.ShapeDtypeStruct((LAYERS, HALF, 128), BF),
        ],
        scratch_shapes=[pltpu.VMEM((128, HALF), I32), pltpu.VMEM((T, FW), F32)],
        compiler_params=params(1),
        name="encode",
    )(active_t, activations, encoder, bias)


def ranks_kernel(table, acts, ranks_out, turned_out, ranks, turned, sent):
    lane = lanes(ROWS)
    bit = lane & 15
    below = lax.shift_left(jnp.full_like(bit, 1), bit) - 1

    @pl.loop(0, LAYERS)
    def _(layer):
        turned[layer] = acts[layer].T

        @pl.loop(0, HALF // ROWS)
        def _(block):
            row = pl.multiple_of(block * ROWS, ROWS)
            entries = table[layer, pl.ds(row, ROWS), :]
            for half in range(2):
                for chunk in range(FW // 128):
                    entry = take(entries, 64 * half + 8 * chunk + right(lane, 4))
                    rank = right(entry, 16) + lax.population_count(entry & below) + 64 * half
                    hit = (right(entry, bit) & 1) == 1
                    place = (layer, pl.ds(row + half * HALF, ROWS), pl.ds(chunk * 128, 128))
                    ranks[place] = jnp.where(hit, rank, -1)

        pltpu.make_async_copy(ranks.at[layer], ranks_out.at[layer], sent.at[layer]).start()
        pltpu.make_async_copy(turned.at[layer], turned_out.at[layer], sent.at[LAYERS + layer]).start()

    @pl.loop(0, LAYERS)
    def _(layer):
        pltpu.make_async_copy(ranks.at[layer], ranks_out.at[layer], sent.at[layer]).wait()
        pltpu.make_async_copy(turned.at[layer], turned_out.at[layer], sent.at[LAYERS + layer]).wait()


def ranks_of(table, activations):
    return pl.pallas_call(
        ranks_kernel,
        in_specs=[HELD, HELD],
        out_specs=[ANY, ANY],
        out_shape=[
            jax.ShapeDtypeStruct((LAYERS, T, FW), I32),
            jax.ShapeDtypeStruct((LAYERS, DW, T), BF),
        ],
        scratch_shapes=[
            pltpu.VMEM((LAYERS, T, FW), I32),
            pltpu.VMEM((LAYERS, DW, T), BF),
            pltpu.SemaphoreType.DMA((2 * LAYERS,)),
        ],
        compiler_params=params(),
        cost_estimate=pl.CostEstimate(flops=4 * 10**9, transcendentals=0, bytes_accessed=12 * 2**20),
        name="ranks",
    )(table, activations)


def each(count, copy, act):
    @pl.loop(0, count)
    def _(i):
        getattr(copy(i), act)()


def rebuild_kernel(ranks_in, slots, decoder, latent_out, own_out, send_out, ranks, latent, total, stage, held, rank_sem, pair_sem, out_sem):
    core = lax.axis_index("lat") % 2

    def load_ranks(layer):
        return pltpu.make_async_copy(ranks_in.at[layer], ranks.at[layer], rank_sem.at[layer])

    def load_pair(p):
        return pltpu.make_async_copy(decoder.at[p], held.at[p], pair_sem.at[p])

    def send_latent(layer):
        return pltpu.make_async_copy(latent.at[layer], latent_out.at[layer], out_sem.at[layer])

    def send_own(i):
        return pltpu.make_async_copy(total.at[core * 4 + i], own_out.at[i], out_sem.at[LAYERS + i])

    def send_other(i):
        return pltpu.make_async_copy(stage.at[i], send_out.at[i], out_sem.at[LAYERS + 4 + i])

    load_ranks(0).start()

    @pl.loop(0, LAYERS)
    def _(source):
        @pl.when(source + 1 < LAYERS)
        def _():
            load_ranks(source + 1).start()

        @pl.loop(source, LAYERS)
        def _(target):
            load_pair(first_pair(source) + target - source).start()

    total[...] = jnp.zeros_like(total)

    @pl.loop(0, LAYERS)
    def _(source):
        load_ranks(source).wait()
        unpack(ranks.at[source], slots.at[source], latent.at[source])
        send_latent(source).start()

        @pl.loop(source, LAYERS)
        def _(target):
            p = first_pair(source) + target - source
            load_pair(p).wait()
            total[target] += jnp.dot(latent[source], held[p], preferred_element_type=F32)

        spot = source % 4

        @pl.when(source // 4 == core)
        def _():
            send_own(spot).start()

        @pl.when(source // 4 != core)
        def _():
            stage[spot] = total[source].astype(BF)
            send_other(spot).start()

    each(LAYERS, send_latent, "wait")
    each(4, send_own, "wait")
    each(4, send_other, "wait")


def rebuild(ranks, slots, decoder):
    return pl.pallas_call(
        rebuild_kernel,
        in_specs=[ANY, HELD, ANY],
        out_specs=[ANY, ANY, ANY],
        out_shape=[
            jax.ShapeDtypeStruct((LAYERS, T, FW), BF),
            jax.ShapeDtypeStruct((4, T, DW), F32),
            jax.ShapeDtypeStruct((4, T, DW), BF),
        ],
        scratch_shapes=[
            pltpu.VMEM((LAYERS, T, FW), I32),
            pltpu.VMEM((LAYERS, T, FW), BF),
            pltpu.VMEM((LAYERS, T, DW), F32),
            pltpu.VMEM((4, T, DW), BF),
            pltpu.VMEM((PAIRS, FW, DW), BF),
            pltpu.SemaphoreType.DMA((LAYERS,)),
            pltpu.SemaphoreType.DMA((PAIRS,)),
            pltpu.SemaphoreType.DMA((2 * LAYERS,)),
        ],
        compiler_params=params(),
        name="rebuild",
    )(ranks, slots, decoder)


def error_loads(mine, other, errors, sems):
    core = lax.axis_index("lat") % 2

    def load(which):
        def at(i):
            spot = (core if which == 0 else 1 - core) * 4 + i
            source = mine if which == 0 else other
            return pltpu.make_async_copy(source.at[i], errors.at[spot], sems.at[which * 4 + i])

        return at

    return load(0), load(1)


def grad_act_kernel(columns, mine, other, decoder, slots_out, errors, total, held, error_sem, pair_sem):
    loads = error_loads(mine, other, errors, error_sem)

    def load_pair(p):
        return pltpu.make_async_copy(decoder.at[p], held.at[p], pair_sem.at[p])

    for load in loads:
        each(4, load, "start")
    each(PAIRS, load_pair, "start")
    for load in loads:
        each(4, load, "wait")

    for source in range(LAYERS):
        for target in range(source, LAYERS):
            p = first_pair(source) + target - source
            load_pair(p).wait()
            part = lax.dot_general(
                errors[target], held[p], (((1,), (1,)), ((), ())), preferred_element_type=F32
            )
            summed = part if target == source else summed + part
        total[...] = summed

        def write(row, packed):
            slots_out[source, pl.ds(row, ROWS), :] = packed

        pack(total, lambda row: columns[source, pl.ds(row, ROWS), :], write)


def grad_act(columns, mine, other, decoder):
    return pl.pallas_call(
        grad_act_kernel,
        in_specs=[HELD, ANY, ANY, ANY],
        out_specs=HELD,
        out_shape=jax.ShapeDtypeStruct((LAYERS, HALF, 128), BF),
        scratch_shapes=[
            pltpu.VMEM((LAYERS, T, DW), BF),
            pltpu.VMEM((T, FW), F32),
            pltpu.VMEM((PAIRS, FW, DW), BF),
            pltpu.SemaphoreType.DMA((LAYERS,)),
            pltpu.SemaphoreType.DMA((PAIRS,)),
        ],
        compiler_params=params(),
        name="grad_act",
    )(columns, mine, other, decoder)


def grad_decoder_part(latent, mine, other, begin, end, earlier=None):
    first, last = first_pair(begin), first_pair(end)
    layers = end - begin

    def kernel(*refs):
        latent_in, mine_in, other_in = refs[:3]
        grad_out, latents, errors, turned, held, latent_sem, error_sem, sent = refs[-8:]
        loads = error_loads(mine_in, other_in, errors, error_sem)

        def load_latent(i):
            return pltpu.make_async_copy(latent_in.at[begin + i], latents.at[i], latent_sem.at[i])

        def send(i):
            return pltpu.make_async_copy(held.at[i], grad_out.at[first + i], sent.at[i])

        load_latent(0).start()
        for load in loads:
            each(4, load, "start")

        @pl.loop(1, layers)
        def _(i):
            load_latent(i).start()

        for load in loads:
            each(4, load, "wait")

        for i in range(layers):
            source = begin + i
            load_latent(i).wait()
            turned[...] = latents[i].T
            for target in range(source, LAYERS):
                at = first_pair(source) + target - source - first
                held[at] = jnp.dot(turned[...], errors[target], preferred_element_type=F32).astype(BF)
                send(at).start()

        each(last - first, send, "wait")

    operands = (latent, mine, other) + (() if earlier is None else (earlier,))
    return pl.pallas_call(
        kernel,
        in_specs=[ANY] * len(operands),
        out_specs=ANY,
        out_shape=jax.ShapeDtypeStruct((PAIRS, FW, DW), BF),
        scratch_shapes=[
            pltpu.VMEM((layers, T, FW), BF),
            pltpu.VMEM((LAYERS, T, DW), BF),
            pltpu.VMEM((FW, T), BF),
            pltpu.VMEM((last - first, FW, DW), BF),
            pltpu.SemaphoreType.DMA((layers,)),
            pltpu.SemaphoreType.DMA((LAYERS,)),
            pltpu.SemaphoreType.DMA((last - first,)),
        ],
        input_output_aliases={} if earlier is None else {3: 0},
        compiler_params=params(),
        cost_estimate=pl.CostEstimate(
            flops=2 * (last - first) * T * FW * DW,
            transcendentals=0,
            bytes_accessed=2 * (last - first) * FW * DW,
        ),
        name=f"grad_decoder_{begin}",
    )(*operands)


def grad_encoder_kernel(ranks_in, slots, turned_in, grad_out, bias_out, ranks, turned, dense, grad, rank_sem, turned_sem, sent):
    def load_ranks(layer):
        return pltpu.make_async_copy(ranks_in.at[layer], ranks.at[layer], rank_sem.at[layer])

    def load_turned(layer):
        return pltpu.make_async_copy(turned_in.at[layer], turned.at[layer], turned_sem.at[layer])

    def send(layer):
        return pltpu.make_async_copy(grad.at[layer], grad_out.at[layer], sent.at[layer])

    @pl.loop(0, LAYERS)
    def _(layer):
        load_ranks(layer).start()
        load_turned(layer).start()

    @pl.loop(0, LAYERS)
    def _(layer):
        load_ranks(layer).wait()
        unpack(ranks.at[layer], slots.at[layer], dense.at[layer])

    for layer in range(LAYERS):
        load_turned(layer).wait()
        grad[layer] = jnp.dot(turned[layer], dense[layer], preferred_element_type=F32).astype(BF)
        send(layer).start()
        bias_out[pl.ds(layer, 1), :] = jnp.sum(dense[layer].astype(F32), axis=0, keepdims=True)

    each(LAYERS, send, "wait")


def grad_encoder_of(ranks, slots, turned):
    return pl.pallas_call(
        grad_encoder_kernel,
        in_specs=[ANY, HELD, ANY],
        out_specs=[ANY, HELD],
        out_shape=[
            jax.ShapeDtypeStruct((LAYERS, DW, FW), BF),
            jax.ShapeDtypeStruct((LAYERS, FW), F32),
        ],
        scratch_shapes=[
            pltpu.VMEM((LAYERS, T, FW), I32),
            pltpu.VMEM((LAYERS, DW, T), BF),
            pltpu.VMEM((LAYERS, T, FW), BF),
            pltpu.VMEM((LAYERS, DW, FW), BF),
            pltpu.SemaphoreType.DMA((LAYERS,)),
            pltpu.SemaphoreType.DMA((LAYERS,)),
            pltpu.SemaphoreType.DMA((LAYERS,)),
        ],
        compiler_params=params(),
        name="grad_encoder",
    )(ranks, slots, turned)


CHIPS = [[2 * chip + core for chip in range(8)] for core in range(2)]


def swap_cores(x):
    return lax.ppermute(x, "lat", [(i, i ^ 1) for i in range(16)])


def over_layer(x):
    return lax.all_to_all(x, "layer", 0, 0, tiled=True)


def over_chips(x):
    return lax.all_to_all(x, "lat", 0, 0, axis_index_groups=CHIPS, tiled=True)


def sum_slots(slots, beside):
    own = jnp.sum(over_layer(slots).astype(F32), axis=0).astype(BF)
    own, beside = lax.optimization_barrier((own, beside))
    return over_layer(jnp.broadcast_to(own[None], slots.shape)), beside


def on_device(activations, targets, encoder, bias, decoder, active):
    lat = lax.axis_index("lat")
    first_row = ((lat % 2) * 8 + lat // 2) * 256
    table, columns, partial = encode(jnp.swapaxes(active, 1, 2), activations, encoder, bias)
    ranks, turned = ranks_of(table, activations)
    latent_slots, ranks = sum_slots(partial, ranks)
    latent, own, send = rebuild(ranks, latent_slots, decoder)
    half = (own + swap_cores(send).astype(F32)).astype(BF).reshape(8, 256, DW)
    total = jnp.sum(over_chips(half).astype(F32), axis=0)
    wanted = lax.dynamic_slice_in_dim(targets.reshape(LAYERS * T, DW), first_row, 256)
    error = (total - wanted.astype(F32)).astype(BF)
    mine = over_chips(jnp.broadcast_to(error[None], (8, 256, DW))).reshape(4, T, DW)
    other = swap_cores(mine)
    grad_slots = grad_act(columns, mine, other, decoder)
    grad_decoder = grad_decoder_part(latent, mine, other, 0, 2)
    grad_slots, grad_decoder = sum_slots(grad_slots, grad_decoder)
    grad_decoder = grad_decoder_part(latent, mine, other, 2, LAYERS, grad_decoder)
    grad_encoder, grad_bias = grad_encoder_of(ranks, grad_slots, turned)
    return (grad_encoder, grad_bias, grad_decoder)


def solution(mesh):
    placed = (
        P(None, None, "layer"),
        P(None, None, "layer"),
        P(None, "layer", "lat"),
        P(None, "lat"),
        P(None, "lat", "layer"),
        P(),
    )
    return jax.shard_map(
        on_device,
        mesh=mesh,
        in_specs=placed,
        out_specs=(P(None, "layer", "lat"), P(None, "lat"), P(None, "lat", "layer")),
        check_vma=False,
    )
```

```python
import jax
import jax.numpy as jnp
from jax import lax
from jax.experimental import pallas as pl
from jax.experimental.pallas import tpu as pltpu
from jax.sharding import PartitionSpec as P

LAYERS = 8
T = 512
HALF = T // 2
DW = 256
FW = 512
ROWS = 256
PAIRS = LAYERS * (LAYERS + 1) // 2
BF = jnp.bfloat16
F32 = jnp.float32
I32 = jnp.int32
ANY = pl.BlockSpec(memory_space=pl.ANY)
HELD = pl.BlockSpec(memory_space=pltpu.VMEM)


def params(steps=0):
    return pltpu.CompilerParams(
        dimension_semantics=("arbitrary",) * steps, vmem_limit_bytes=60 * 1024 * 1024
    )


def first_pair(source):
    return source * LAYERS - source * (source - 1) // 2


def take(x, index):
    return jnp.take_along_axis(x, index, axis=1)


def lanes(rows):
    return lax.broadcasted_iota(I32, (rows, 128), 1)


def right(x, by):
    return lax.shift_right_logical(x, jnp.full_like(x, by) if isinstance(by, int) else by)


def pack(dense, columns_at, write):
    lane = lanes(ROWS)

    @pl.loop(0, HALF // ROWS)
    def _(block):
        row = pl.multiple_of(block * ROWS, ROWS)
        columns = columns_at(row) & (FW - 1)
        within = columns & 127
        chunk_of = right(columns, 7)
        packed = None
        for chunk in range(FW // 128):
            part = pl.ds(chunk * 128, 128)
            low = take(dense[pl.ds(row, ROWS), part], within)
            high = take(dense[pl.ds(row + HALF, ROWS), part], within)
            picked = jnp.where(lane < 64, low, high)
            packed = picked if packed is None else jnp.where(chunk_of == chunk, picked, packed)
        write(row, packed.astype(BF))


def unpack(ranks, slots, dense):
    @pl.loop(0, HALF // ROWS)
    def _(block):
        row = pl.multiple_of(block * ROWS, ROWS)
        values = slots[pl.ds(row, ROWS), :].astype(F32)
        for half in range(2):
            for chunk in range(FW // 128):
                place = (pl.ds(row + half * HALF, ROWS), pl.ds(chunk * 128, 128))
                rank = ranks[place]
                value = jnp.where(rank >= 0, take(values, rank & 127), 0.0)
                dense[place] = value.astype(BF)


def unpack_next(ranks, slots, dense, layer, part, parts):
    places = [(half, chunk) for half in range(2) for chunk in range(FW // 128)]
    count = len(places)
    for half, chunk in places[count * part // parts : count * (part + 1) // parts]:
        place = (layer, pl.ds(half * HALF, HALF), pl.ds(chunk * 128, 128))
        rank = ranks[place]
        value = jnp.where(rank >= 0, take(slots[layer].astype(F32), rank & 127), 0.0)
        dense[place] = value.astype(BF)


def encode_kernel(active, acts, encoder, bias, columns_out, slots_out, rows, dense):
    layer = pl.program_id(0)
    rel = active[0] - lax.axis_index("lat") * FW
    rows[0:64, :] = rel[:, :HALF]
    rows[64:128, :] = rel[:, HALF:]
    columns_out[0] = rows[...].T
    added = jnp.where(lax.axis_index("layer") == 0, 1.0, 0.0).astype(F32)
    value = jnp.dot(acts[0], encoder[0], preferred_element_type=F32)
    dense[...] = value + bias[pl.ds(layer, 1), :] * added

    def write(row, packed):
        slots_out[0, pl.ds(row, ROWS), :] = packed

    pack(dense, lambda row: columns_out[0, pl.ds(row, ROWS), :], write)


def one(*shape):
    return pl.BlockSpec((1,) + shape, lambda i: (i,) + (0,) * len(shape))


def whole(*shape):
    return pl.BlockSpec(shape, lambda i: (0,) * len(shape))


def encode(active_t, activations, encoder, bias):
    return pl.pallas_call(
        encode_kernel,
        grid=(LAYERS,),
        in_specs=[one(64, T), one(T, DW), one(DW, FW), whole(LAYERS, FW)],
        out_specs=[one(HALF, 128), one(HALF, 128)],
        out_shape=[
            jax.ShapeDtypeStruct((LAYERS, HALF, 128), I32),
            jax.ShapeDtypeStruct((LAYERS, HALF, 128), BF),
        ],
        scratch_shapes=[pltpu.VMEM((128, HALF), I32), pltpu.VMEM((T, FW), F32)],
        compiler_params=params(1),
        name="encode",
    )(active_t, activations, encoder, bias)


def ranks_kernel(active, columns, ranks_out, order_out, rows, table, ranks, sent):
    lane = lanes(ROWS)
    bit = lane & 15
    below = lax.shift_left(jnp.full_like(bit, 1), bit) - 1
    own = lax.axis_index("layer")
    first = lax.axis_index("lat") * FW
    rows[...] = jnp.zeros_like(rows)

    def send(layer):
        return pltpu.make_async_copy(ranks.at[layer], ranks_out.at[layer], sent.at[layer])

    @pl.loop(0, LAYERS)
    def _(layer):
        rel = active[layer] - first
        high = lax.shift_right_arithmetic(rel, jnp.full_like(rel, 5))
        bits = lax.shift_left(jnp.full_like(rel, 1), rel & 31)
        before = jnp.zeros((1, T), I32)
        for word in range(16):
            marked = jnp.where(high == word, bits, 0)
            folded = marked[0:8]
            for k in range(8, 64, 8):
                folded = folded | marked[k : k + 8]
            both = jnp.sum(folded, axis=0, keepdims=True)
            for part in range(2):
                piece = both & 0xFFFF if part == 0 else right(both, 16)
                entry = piece | lax.shift_left(before, jnp.full_like(before, 16))
                before = before + lax.population_count(piece)
                for half in range(2):
                    at = 64 * half + 2 * word + part
                    rows[at : at + 1, :] = entry[:, half * HALF : (half + 1) * HALF]
        entries = rows[...].T

        @pl.when(layer == own)
        def _():
            table[...] = entries

        for half in range(2):
            for chunk in range(FW // 128):
                entry = take(entries, 64 * half + 8 * chunk + right(lane, 4))
                rank = right(entry, 16) + lax.population_count(entry & below) + 64 * half
                hit = (right(entry, bit) & 1) == 1
                place = (layer, pl.ds(half * HALF, HALF), pl.ds(chunk * 128, 128))
                ranks[place] = jnp.where(hit, rank, -1)
        send(layer).start()

    column = columns[own]
    held = (column >= 0) & (column < FW)
    column = column & (FW - 1)
    entry = take(table[...], (lane & 64) + right(column, 4))
    under = lax.shift_left(jnp.full_like(column, 1), column & 15) - 1
    rank = right(entry, 16) + lax.population_count(entry & under)
    turned = jnp.where(held, rank, -1).T
    slot = lax.broadcasted_iota(I32, (64, HALF), 0)
    for half in range(2):
        mine = turned[64 * half : 64 * half + 64]
        for r in range(64):
            at = 64 * half + r
            rows[at : at + 1, :] = 64 * half + jnp.sum(
                jnp.where(mine == r, slot, 0), axis=0, keepdims=True
            )
    order_out[...] = rows[...].T
    each(LAYERS, send, "wait")


def ranks_of(active_t, columns):
    return pl.pallas_call(
        ranks_kernel,
        in_specs=[HELD, HELD],
        out_specs=[ANY, HELD],
        out_shape=[
            jax.ShapeDtypeStruct((LAYERS, T, FW), I32),
            jax.ShapeDtypeStruct((HALF, 128), I32),
        ],
        scratch_shapes=[
            pltpu.VMEM((128, HALF), I32),
            pltpu.VMEM((HALF, 128), I32),
            pltpu.VMEM((LAYERS, T, FW), I32),
            pltpu.SemaphoreType.DMA((LAYERS,)),
        ],
        compiler_params=params(),
        cost_estimate=pl.CostEstimate(flops=5 * 10**9, transcendentals=0, bytes_accessed=10 * 2**20),
        name="ranks",
    )(active_t, columns)


def turn_kernel(acts, out):
    for layer in range(LAYERS):
        out[layer] = acts[layer].T


def turn(activations):
    return pl.pallas_call(
        turn_kernel,
        in_specs=[HELD],
        out_specs=HELD,
        out_shape=jax.ShapeDtypeStruct((LAYERS, DW, T), BF),
        compiler_params=params(),
        cost_estimate=pl.CostEstimate(flops=10**9, transcendentals=0, bytes_accessed=4 * 2**20),
        name="turn",
    )(activations)


def settle_kernel(parts, order, out):
    own = parts[0].astype(F32)
    for i in range(1, LAYERS):
        own = own + parts[i].astype(F32)
    own = take(own, order[...]).astype(BF)
    for i in range(LAYERS):
        out[i] = own


def settle(parts, order):
    return pl.pallas_call(
        settle_kernel,
        in_specs=[HELD, HELD],
        out_specs=HELD,
        out_shape=jax.ShapeDtypeStruct((LAYERS, HALF, 128), BF),
        compiler_params=params(),
        name="settle",
    )(parts, order)


def each(count, copy, act):
    @pl.loop(0, count)
    def _(i):
        getattr(copy(i), act)()


def rebuild_kernel(ranks_in, slots, decoder, latent_out, own_out, send_out, ranks, latent, total, stage, held, rank_sem, pair_sem, out_sem):
    core = lax.axis_index("lat") % 2

    def load_ranks(layer):
        return pltpu.make_async_copy(ranks_in.at[layer], ranks.at[layer], rank_sem.at[layer])

    def load_pair(p):
        return pltpu.make_async_copy(decoder.at[p], held.at[p], pair_sem.at[p])

    def send_latent(layer):
        return pltpu.make_async_copy(latent.at[layer], latent_out.at[layer], out_sem.at[layer])

    def send_own(i):
        return pltpu.make_async_copy(total.at[core * 4 + i], own_out.at[i], out_sem.at[LAYERS + i])

    def send_other(i):
        return pltpu.make_async_copy(stage.at[i], send_out.at[i], out_sem.at[LAYERS + 4 + i])

    load_ranks(0).start()

    @pl.loop(0, LAYERS)
    def _(source):
        @pl.when(source + 1 < LAYERS)
        def _():
            load_ranks(source + 1).start()

        @pl.loop(source, LAYERS)
        def _(target):
            load_pair(first_pair(source) + target - source).start()

    load_ranks(0).wait()
    unpack(ranks.at[0], slots.at[0], latent.at[0])
    for source in range(LAYERS):
        if source + 1 < LAYERS:
            load_ranks(source + 1).wait()
        for target in range(source, LAYERS):
            load_pair(first_pair(source) + target - source).wait()
        send_latent(source).start()
        count = LAYERS - source
        for i, target in enumerate(range(source, LAYERS)):
            p = first_pair(source) + target - source
            part = jnp.dot(latent[source], held[p], preferred_element_type=F32)
            total[target] = part if source == 0 else total[target] + part
            if source + 1 < LAYERS:
                unpack_next(ranks, slots, latent, source + 1, i, count)

        spot = source % 4

        @pl.when(source // 4 == core)
        def _(spot=spot):
            send_own(spot).start()

        @pl.when(source // 4 != core)
        def _(spot=spot, source=source):
            stage[spot] = total[source].astype(BF)
            send_other(spot).start()

    each(LAYERS, send_latent, "wait")
    each(4, send_own, "wait")
    each(4, send_other, "wait")


def rebuild(ranks, slots, decoder):
    return pl.pallas_call(
        rebuild_kernel,
        in_specs=[ANY, HELD, ANY],
        out_specs=[ANY, ANY, ANY],
        out_shape=[
            jax.ShapeDtypeStruct((LAYERS, T, FW), BF),
            jax.ShapeDtypeStruct((4, T, DW), F32),
            jax.ShapeDtypeStruct((4, T, DW), BF),
        ],
        scratch_shapes=[
            pltpu.VMEM((LAYERS, T, FW), I32),
            pltpu.VMEM((LAYERS, T, FW), BF),
            pltpu.VMEM((LAYERS, T, DW), F32),
            pltpu.VMEM((4, T, DW), BF),
            pltpu.VMEM((PAIRS, FW, DW), BF),
            pltpu.SemaphoreType.DMA((LAYERS,)),
            pltpu.SemaphoreType.DMA((PAIRS,)),
            pltpu.SemaphoreType.DMA((2 * LAYERS,)),
        ],
        compiler_params=params(),
        name="rebuild",
    )(ranks, slots, decoder)


def error_loads(mine, other, errors, sems):
    core = lax.axis_index("lat") % 2

    def load(which):
        def at(i):
            spot = (core if which == 0 else 1 - core) * 4 + i
            source = mine if which == 0 else other
            return pltpu.make_async_copy(source.at[i], errors.at[spot], sems.at[which * 4 + i])

        return at

    return load(0), load(1)


def grad_act_kernel(columns, mine, other, decoder, slots_out, errors, total, held, error_sem, pair_sem):
    loads = error_loads(mine, other, errors, error_sem)

    def load_pair(p):
        return pltpu.make_async_copy(decoder.at[p], held.at[p], pair_sem.at[p])

    for load in loads:
        each(4, load, "start")
    each(PAIRS, load_pair, "start")
    for load in loads:
        each(4, load, "wait")

    for source in range(LAYERS):
        for target in range(source, LAYERS):
            p = first_pair(source) + target - source
            load_pair(p).wait()
            part = lax.dot_general(
                errors[target], held[p], (((1,), (1,)), ((), ())), preferred_element_type=F32
            )
            summed = part if target == source else summed + part
        total[...] = summed

        def write(row, packed):
            slots_out[source, pl.ds(row, ROWS), :] = packed

        pack(total, lambda row: columns[source, pl.ds(row, ROWS), :], write)


def grad_act(columns, mine, other, decoder):
    return pl.pallas_call(
        grad_act_kernel,
        in_specs=[HELD, ANY, ANY, ANY],
        out_specs=HELD,
        out_shape=jax.ShapeDtypeStruct((LAYERS, HALF, 128), BF),
        scratch_shapes=[
            pltpu.VMEM((LAYERS, T, DW), BF),
            pltpu.VMEM((T, FW), F32),
            pltpu.VMEM((PAIRS, FW, DW), BF),
            pltpu.SemaphoreType.DMA((LAYERS,)),
            pltpu.SemaphoreType.DMA((PAIRS,)),
        ],
        compiler_params=params(),
        name="grad_act",
    )(columns, mine, other, decoder)


def grad_decoder_part(latent, mine, other, begin, end, earlier=None):
    first, last = first_pair(begin), first_pair(end)
    layers = end - begin

    def kernel(*refs):
        latent_in, mine_in, other_in = refs[:3]
        grad_out, latents, errors, turned, held, latent_sem, error_sem, sent = refs[-8:]
        loads = error_loads(mine_in, other_in, errors, error_sem)

        def load_latent(i):
            return pltpu.make_async_copy(latent_in.at[begin + i], latents.at[i], latent_sem.at[i])

        def send(i):
            return pltpu.make_async_copy(held.at[i], grad_out.at[first + i], sent.at[i])

        load_latent(0).start()
        for load in loads:
            each(4, load, "start")

        @pl.loop(1, layers)
        def _(i):
            load_latent(i).start()

        for load in loads:
            each(4, load, "wait")

        for i in range(layers):
            source = begin + i
            load_latent(i).wait()
            turned[...] = latents[i].T
            for target in range(source, LAYERS):
                at = first_pair(source) + target - source - first
                held[at] = jnp.dot(turned[...], errors[target], preferred_element_type=F32).astype(BF)
                send(at).start()

        each(last - first, send, "wait")

    operands = (latent, mine, other) + (() if earlier is None else (earlier,))
    return pl.pallas_call(
        kernel,
        in_specs=[ANY] * len(operands),
        out_specs=ANY,
        out_shape=jax.ShapeDtypeStruct((PAIRS, FW, DW), BF),
        scratch_shapes=[
            pltpu.VMEM((layers, T, FW), BF),
            pltpu.VMEM((LAYERS, T, DW), BF),
            pltpu.VMEM((FW, T), BF),
            pltpu.VMEM((last - first, FW, DW), BF),
            pltpu.SemaphoreType.DMA((layers,)),
            pltpu.SemaphoreType.DMA((LAYERS,)),
            pltpu.SemaphoreType.DMA((last - first,)),
        ],
        input_output_aliases={} if earlier is None else {3: 0},
        compiler_params=params(),
        cost_estimate=pl.CostEstimate(
            flops=2 * (last - first) * T * FW * DW,
            transcendentals=0,
            bytes_accessed=2 * (last - first) * FW * DW,
        ),
        name=f"grad_decoder_{begin}",
    )(*operands)


def grad_encoder_kernel(ranks_in, slots, turned_in, grad_out, bias_out, ranks, turned, dense, grad, rank_sem, turned_sem, sent):
    def load_ranks(layer):
        return pltpu.make_async_copy(ranks_in.at[layer], ranks.at[layer], rank_sem.at[layer])

    def load_turned(layer):
        return pltpu.make_async_copy(turned_in.at[layer], turned.at[layer], turned_sem.at[layer])

    def send(layer):
        return pltpu.make_async_copy(grad.at[layer], grad_out.at[layer], sent.at[layer])

    @pl.loop(0, LAYERS)
    def _(layer):
        load_ranks(layer).start()
        load_turned(layer).start()

    load_ranks(0).wait()
    unpack(ranks.at[0], slots.at[0], dense.at[0])
    for layer in range(LAYERS):
        load_turned(layer).wait()
        if layer + 1 < LAYERS:
            load_ranks(layer + 1).wait()
            unpack_next(ranks, slots, dense, layer + 1, 0, 1)
        grad[layer] = jnp.dot(turned[layer], dense[layer], preferred_element_type=F32).astype(BF)
        bias_out[layer : layer + 1, :] = jnp.dot(
            jnp.ones((16, T), BF), dense[layer], preferred_element_type=F32
        )[0:1]
        send(layer).start()

    each(LAYERS, send, "wait")


def grad_encoder_of(ranks, slots, turned):
    return pl.pallas_call(
        grad_encoder_kernel,
        in_specs=[ANY, HELD, ANY],
        out_specs=[ANY, HELD],
        out_shape=[
            jax.ShapeDtypeStruct((LAYERS, DW, FW), BF),
            jax.ShapeDtypeStruct((LAYERS, FW), F32),
        ],
        scratch_shapes=[
            pltpu.VMEM((LAYERS, T, FW), I32),
            pltpu.VMEM((LAYERS, DW, T), BF),
            pltpu.VMEM((LAYERS, T, FW), BF),
            pltpu.VMEM((LAYERS, DW, FW), BF),
            pltpu.SemaphoreType.DMA((LAYERS,)),
            pltpu.SemaphoreType.DMA((LAYERS,)),
            pltpu.SemaphoreType.DMA((LAYERS,)),
        ],
        compiler_params=params(),
        name="grad_encoder",
    )(ranks, slots, turned)


CHIPS = [[2 * chip + core for chip in range(8)] for core in range(2)]


def swap_cores(x):
    return lax.ppermute(x, "lat", [(i, i ^ 1) for i in range(16)])


def over_layer(x):
    return lax.all_to_all(x, "layer", 0, 0, tiled=True)


def over_chips(x):
    return lax.all_to_all(x, "lat", 0, 0, axis_index_groups=CHIPS, tiled=True)


def on_device(activations, targets, encoder, bias, decoder, active):
    lat = lax.axis_index("lat")
    first_row = ((lat % 2) * 8 + lat // 2) * 256
    active_t = jnp.swapaxes(active, 1, 2)
    columns, partial = encode(active_t, activations, encoder, bias)
    ranks, order = ranks_of(active_t, columns)
    settled = settle(over_layer(partial), order)
    settled, late = lax.optimization_barrier((settled, activations))
    turned = turn(late)
    latent, own, send = rebuild(ranks, over_layer(settled), decoder)
    half = (own + swap_cores(send).astype(F32)).astype(BF).reshape(8, 256, DW)
    total = jnp.sum(over_chips(half).astype(F32), axis=0)
    wanted = lax.dynamic_slice_in_dim(targets.reshape(LAYERS * T, DW), first_row, 256)
    error = (total - wanted.astype(F32)).astype(BF)
    mine = over_chips(jnp.broadcast_to(error[None], (8, 256, DW))).reshape(4, T, DW)
    other = swap_cores(mine)
    parts = over_layer(grad_act(columns, mine, other, decoder))
    grad_decoder = grad_decoder_part(latent, mine, other, 0, 3)
    parts, grad_decoder = lax.optimization_barrier((parts, grad_decoder))
    settled = over_layer(settle(parts, order))
    grad_decoder = grad_decoder_part(latent, mine, other, 3, LAYERS, grad_decoder)
    grad_encoder, grad_bias = grad_encoder_of(ranks, settled, turned)
    return (grad_encoder, grad_bias, grad_decoder)


def solution(mesh):
    placed = (
        P(None, None, "layer"),
        P(None, None, "layer"),
        P(None, "layer", "lat"),
        P(None, "lat"),
        P(None, "lat", "layer"),
        P(),
    )
    return jax.shard_map(
        on_device,
        mesh=mesh,
        in_specs=placed,
        out_specs=(P(None, "layer", "lat"), P(None, "lat"), P(None, "lat", "layer")),
        check_vma=False,
    )
```

```python
import jax
import jax.numpy as jnp
from jax import lax
from jax.experimental import pallas as pl
from jax.experimental.pallas import tpu as pltpu
from jax.sharding import PartitionSpec as P

LAYERS = 8
T = 512
HALF = T // 2
DW = 256
FW = 512
ROWS = 256
PAIRS = LAYERS * (LAYERS + 1) // 2
BF = jnp.bfloat16
F32 = jnp.float32
I32 = jnp.int32
ANY = pl.BlockSpec(memory_space=pl.ANY)
HELD = pl.BlockSpec(memory_space=pltpu.VMEM)


def params(steps=0):
    return pltpu.CompilerParams(
        dimension_semantics=("arbitrary",) * steps, vmem_limit_bytes=60 * 1024 * 1024
    )


def first_pair(source):
    return source * LAYERS - source * (source - 1) // 2


def take(x, index):
    return jnp.take_along_axis(x, index, axis=1)


def lanes(rows):
    return lax.broadcasted_iota(I32, (rows, 128), 1)


def right(x, by):
    return lax.shift_right_logical(x, jnp.full_like(x, by) if isinstance(by, int) else by)


def pack_rows(dense, columns, row, write):
    lane = lanes(ROWS)
    columns = columns & (FW - 1)
    within = columns & 127
    chunk_of = right(columns, 7)
    packed = None
    for chunk in range(FW // 128):
        part = pl.ds(chunk * 128, 128)
        low = take(dense[pl.ds(row, ROWS), part], within)
        high = take(dense[pl.ds(row + HALF, ROWS), part], within)
        picked = jnp.where(lane < 64, low, high)
        packed = picked if packed is None else jnp.where(chunk_of == chunk, picked, packed)
    write(row, packed.astype(BF))


def pack(dense, columns_at, write):
    @pl.loop(0, HALF // ROWS)
    def _(block):
        row = pl.multiple_of(block * ROWS, ROWS)
        pack_rows(dense, columns_at(row), row, write)


def unpack(ranks, slots, dense):
    @pl.loop(0, HALF // ROWS)
    def _(block):
        row = pl.multiple_of(block * ROWS, ROWS)
        values = slots[pl.ds(row, ROWS), :].astype(F32)
        for half in range(2):
            for chunk in range(FW // 128):
                place = (pl.ds(row + half * HALF, ROWS), pl.ds(chunk * 128, 128))
                rank = ranks[place]
                value = jnp.where(rank >= 0, take(values, rank & 127), 0.0)
                dense[place] = value.astype(BF)


def unpack_next(ranks, slots, dense, layer, part, parts):
    places = [(half, chunk) for half in range(2) for chunk in range(FW // 128)]
    count = len(places)
    for half, chunk in places[count * part // parts : count * (part + 1) // parts]:
        place = (layer, pl.ds(half * HALF, HALF), pl.ds(chunk * 128, 128))
        rank = ranks[place]
        value = jnp.where(rank >= 0, take(slots[layer].astype(F32), rank & 127), 0.0)
        dense[place] = value.astype(BF)


def encode_kernel(active, acts, encoder, bias, columns_out, slots_out, rows, dense):
    layer = pl.program_id(0)
    rel = active[0] - lax.axis_index("lat") * FW
    rows[0:64, :] = rel[:, :HALF]
    rows[64:128, :] = rel[:, HALF:]
    columns_out[0] = rows[...].T
    added = jnp.where(lax.axis_index("layer") == 0, 1.0, 0.0).astype(F32)
    value = jnp.dot(acts[0], encoder[0], preferred_element_type=F32)
    dense[...] = value + bias[pl.ds(layer, 1), :] * added

    def write(row, packed):
        slots_out[0, pl.ds(row, ROWS), :] = packed

    pack(dense, lambda row: columns_out[0, pl.ds(row, ROWS), :], write)


def one(*shape):
    return pl.BlockSpec((1,) + shape, lambda i: (i,) + (0,) * len(shape))


def whole(*shape):
    return pl.BlockSpec(shape, lambda i: (0,) * len(shape))


def encode(active_t, activations, encoder, bias):
    return pl.pallas_call(
        encode_kernel,
        grid=(LAYERS,),
        in_specs=[one(64, T), one(T, DW), one(DW, FW), whole(LAYERS, FW)],
        out_specs=[one(HALF, 128), one(HALF, 128)],
        out_shape=[
            jax.ShapeDtypeStruct((LAYERS, HALF, 128), I32),
            jax.ShapeDtypeStruct((LAYERS, HALF, 128), BF),
        ],
        scratch_shapes=[pltpu.VMEM((128, HALF), I32), pltpu.VMEM((T, FW), F32)],
        compiler_params=params(1),
        name="encode",
    )(active_t, activations, encoder, bias)


def ranks_kernel(active, columns, ranks_out, order_out, rows, table, ranks, sent):
    lane = lanes(ROWS)
    bit = lane & 15
    below = lax.shift_left(jnp.full_like(bit, 1), bit) - 1
    own = lax.axis_index("layer")
    first = lax.axis_index("lat") * FW
    rows[...] = jnp.zeros_like(rows)

    def send(layer):
        return pltpu.make_async_copy(ranks.at[layer], ranks_out.at[layer], sent.at[layer])

    @pl.loop(0, LAYERS)
    def _(layer):
        rel = active[layer] - first
        high = lax.shift_right_arithmetic(rel, jnp.full_like(rel, 5))
        bits = lax.shift_left(jnp.full_like(rel, 1), rel & 31)
        before = jnp.zeros((1, T), I32)
        for word in range(16):
            marked = jnp.where(high == word, bits, 0)
            folded = marked[0:8]
            for k in range(8, 64, 8):
                folded = folded | marked[k : k + 8]
            both = jnp.sum(folded, axis=0, keepdims=True)
            for part in range(2):
                piece = both & 0xFFFF if part == 0 else right(both, 16)
                entry = piece | lax.shift_left(before, jnp.full_like(before, 16))
                before = before + lax.population_count(piece)
                for half in range(2):
                    at = 64 * half + 2 * word + part
                    rows[at : at + 1, :] = entry[:, half * HALF : (half + 1) * HALF]
        entries = rows[...].T

        @pl.when(layer == own)
        def _():
            table[...] = entries

        for half in range(2):
            for chunk in range(FW // 128):
                entry = take(entries, 64 * half + 8 * chunk + right(lane, 4))
                rank = right(entry, 16) + lax.population_count(entry & below) + 64 * half
                hit = (right(entry, bit) & 1) == 1
                place = (layer, pl.ds(half * HALF, HALF), pl.ds(chunk * 128, 128))
                ranks[place] = jnp.where(hit, rank, -1)
        send(layer).start()

    column = columns[own]
    held = (column >= 0) & (column < FW)
    column = column & (FW - 1)
    entry = take(table[...], (lane & 64) + right(column, 4))
    under = lax.shift_left(jnp.full_like(column, 1), column & 15) - 1
    rank = right(entry, 16) + lax.population_count(entry & under)
    turned = jnp.where(held, rank, -1).T
    slot = lax.broadcasted_iota(I32, (64, HALF), 0)
    for half in range(2):
        mine = turned[64 * half : 64 * half + 64]
        for r in range(64):
            at = 64 * half + r
            rows[at : at + 1, :] = 64 * half + jnp.sum(
                jnp.where(mine == r, slot, 0), axis=0, keepdims=True
            )
    order_out[...] = rows[...].T
    each(LAYERS, send, "wait")


def ranks_of(active_t, columns):
    return pl.pallas_call(
        ranks_kernel,
        in_specs=[HELD, HELD],
        out_specs=[ANY, HELD],
        out_shape=[
            jax.ShapeDtypeStruct((LAYERS, T, FW), I32),
            jax.ShapeDtypeStruct((HALF, 128), I32),
        ],
        scratch_shapes=[
            pltpu.VMEM((128, HALF), I32),
            pltpu.VMEM((HALF, 128), I32),
            pltpu.VMEM((LAYERS, T, FW), I32),
            pltpu.SemaphoreType.DMA((LAYERS,)),
        ],
        compiler_params=params(),
        cost_estimate=pl.CostEstimate(flops=5 * 10**9, transcendentals=0, bytes_accessed=10 * 2**20),
        name="ranks",
    )(active_t, columns)


def turn_kernel(acts, out):
    for layer in range(LAYERS):
        out[layer] = acts[layer].T


def turn(activations):
    return pl.pallas_call(
        turn_kernel,
        in_specs=[HELD],
        out_specs=HELD,
        out_shape=jax.ShapeDtypeStruct((LAYERS, DW, T), BF),
        compiler_params=params(),
        cost_estimate=pl.CostEstimate(flops=10**9, transcendentals=0, bytes_accessed=4 * 2**20),
        name="turn",
    )(activations)


def settle_kernel(parts, order, out):
    own = parts[0].astype(F32)
    for i in range(1, LAYERS):
        own = own + parts[i].astype(F32)
    own = take(own, order[...]).astype(BF)
    for i in range(LAYERS):
        out[i] = own


def settle(parts, order):
    return pl.pallas_call(
        settle_kernel,
        in_specs=[HELD, HELD],
        out_specs=HELD,
        out_shape=jax.ShapeDtypeStruct((LAYERS, HALF, 128), BF),
        compiler_params=params(),
        name="settle",
    )(parts, order)


def each(count, copy, act):
    @pl.loop(0, count)
    def _(i):
        getattr(copy(i), act)()


def rebuild_kernel(ranks_in, slots, decoder, latent_out, own_out, send_out, ranks, latent, total, stage, held, rank_sem, pair_sem, out_sem):
    core = lax.axis_index("lat") % 2

    def load_ranks(layer):
        return pltpu.make_async_copy(ranks_in.at[layer], ranks.at[layer], rank_sem.at[layer])

    def load_pair(p):
        return pltpu.make_async_copy(decoder.at[p], held.at[p], pair_sem.at[p])

    def send_latent(layer):
        return pltpu.make_async_copy(latent.at[layer], latent_out.at[layer], out_sem.at[layer])

    def send_own(i):
        return pltpu.make_async_copy(total.at[core * 4 + i], own_out.at[i], out_sem.at[LAYERS + i])

    def send_other(i):
        return pltpu.make_async_copy(stage.at[i], send_out.at[i], out_sem.at[LAYERS + 4 + i])

    load_ranks(0).start()

    @pl.loop(0, LAYERS)
    def _(source):
        @pl.when(source + 1 < LAYERS)
        def _():
            load_ranks(source + 1).start()

        @pl.loop(source, LAYERS)
        def _(target):
            load_pair(first_pair(source) + target - source).start()

    load_ranks(0).wait()
    unpack(ranks.at[0], slots.at[0], latent.at[0])
    for source in range(LAYERS):
        if source + 1 < LAYERS:
            load_ranks(source + 1).wait()
        for target in range(source, LAYERS):
            load_pair(first_pair(source) + target - source).wait()
        send_latent(source).start()
        count = LAYERS - source
        for i, target in enumerate(range(source, LAYERS)):
            p = first_pair(source) + target - source
            part = jnp.dot(latent[source], held[p], preferred_element_type=F32)
            total[target] = part if source == 0 else total[target] + part
            if source + 1 < LAYERS:
                unpack_next(ranks, slots, latent, source + 1, i, count)

        spot = source % 4

        @pl.when(source // 4 == core)
        def _(spot=spot):
            send_own(spot).start()

        @pl.when(source // 4 != core)
        def _(spot=spot, source=source):
            stage[spot] = total[source].astype(BF)
            send_other(spot).start()

    each(LAYERS, send_latent, "wait")
    each(4, send_own, "wait")
    each(4, send_other, "wait")


def rebuild(ranks, slots, decoder):
    return pl.pallas_call(
        rebuild_kernel,
        in_specs=[ANY, HELD, ANY],
        out_specs=[ANY, ANY, ANY],
        out_shape=[
            jax.ShapeDtypeStruct((LAYERS, T, FW), BF),
            jax.ShapeDtypeStruct((4, T, DW), F32),
            jax.ShapeDtypeStruct((4, T, DW), BF),
        ],
        scratch_shapes=[
            pltpu.VMEM((LAYERS, T, FW), I32),
            pltpu.VMEM((LAYERS, T, FW), BF),
            pltpu.VMEM((LAYERS, T, DW), F32),
            pltpu.VMEM((4, T, DW), BF),
            pltpu.VMEM((PAIRS, FW, DW), BF),
            pltpu.SemaphoreType.DMA((LAYERS,)),
            pltpu.SemaphoreType.DMA((PAIRS,)),
            pltpu.SemaphoreType.DMA((2 * LAYERS,)),
        ],
        compiler_params=params(),
        name="rebuild",
    )(ranks, slots, decoder)


def error_loads(mine, other, errors, sems):
    core = lax.axis_index("lat") % 2

    def load(which):
        def at(i):
            spot = (core if which == 0 else 1 - core) * 4 + i
            source = mine if which == 0 else other
            return pltpu.make_async_copy(source.at[i], errors.at[spot], sems.at[which * 4 + i])

        return at

    return load(0), load(1)


def grad_act_kernel(columns, mine, other, decoder, slots_out, errors, total, held, error_sem, pair_sem):
    loads = error_loads(mine, other, errors, error_sem)

    def load_pair(p):
        return pltpu.make_async_copy(decoder.at[p], held.at[p], pair_sem.at[p])

    for load in loads:
        each(4, load, "start")
    each(PAIRS, load_pair, "start")
    for load in loads:
        each(4, load, "wait")

    def pack_layer(layer):
        def write(row, packed):
            slots_out[layer, pl.ds(row, ROWS), :] = packed

        pack_rows(total.at[layer % 2], columns[layer], 0, write)

    for source in range(LAYERS):
        for target in range(source, LAYERS):
            load_pair(first_pair(source) + target - source).wait()
        summed = None
        for target in range(source, LAYERS):
            part = lax.dot_general(
                errors[target],
                held[first_pair(source) + target - source],
                (((1,), (1,)), ((), ())),
                preferred_element_type=F32,
            )
            summed = part if summed is None else summed + part
        total[source % 2] = summed
        if source > 0:
            pack_layer(source - 1)
    pack_layer(LAYERS - 1)


def grad_act(columns, mine, other, decoder):
    return pl.pallas_call(
        grad_act_kernel,
        in_specs=[HELD, ANY, ANY, ANY],
        out_specs=HELD,
        out_shape=jax.ShapeDtypeStruct((LAYERS, HALF, 128), BF),
        scratch_shapes=[
            pltpu.VMEM((LAYERS, T, DW), BF),
            pltpu.VMEM((2, T, FW), F32),
            pltpu.VMEM((PAIRS, FW, DW), BF),
            pltpu.SemaphoreType.DMA((LAYERS,)),
            pltpu.SemaphoreType.DMA((PAIRS,)),
        ],
        compiler_params=params(),
        name="grad_act",
    )(columns, mine, other, decoder)


def grad_decoder_part(latent, mine, other, begin, end, earlier=None):
    first, last = first_pair(begin), first_pair(end)
    layers = end - begin

    def kernel(*refs):
        latent_in, mine_in, other_in = refs[:3]
        grad_out, latents, errors, turned, held, latent_sem, error_sem, sent = refs[-8:]
        loads = error_loads(mine_in, other_in, errors, error_sem)

        def load_latent(i):
            return pltpu.make_async_copy(latent_in.at[begin + i], latents.at[i], latent_sem.at[i])

        def send(i):
            return pltpu.make_async_copy(held.at[i], grad_out.at[first + i], sent.at[i])

        load_latent(0).start()
        for load in loads:
            each(4, load, "start")

        @pl.loop(1, layers)
        def _(i):
            load_latent(i).start()

        for load in loads:
            each(4, load, "wait")

        for i in range(layers):
            source = begin + i
            load_latent(i).wait()
            turned[...] = latents[i].T
            for target in range(source, LAYERS):
                at = first_pair(source) + target - source - first
                held[at] = jnp.dot(turned[...], errors[target], preferred_element_type=F32).astype(BF)
                send(at).start()

        each(last - first, send, "wait")

    operands = (latent, mine, other) + (() if earlier is None else (earlier,))
    return pl.pallas_call(
        kernel,
        in_specs=[ANY] * len(operands),
        out_specs=ANY,
        out_shape=jax.ShapeDtypeStruct((PAIRS, FW, DW), BF),
        scratch_shapes=[
            pltpu.VMEM((layers, T, FW), BF),
            pltpu.VMEM((LAYERS, T, DW), BF),
            pltpu.VMEM((FW, T), BF),
            pltpu.VMEM((last - first, FW, DW), BF),
            pltpu.SemaphoreType.DMA((layers,)),
            pltpu.SemaphoreType.DMA((LAYERS,)),
            pltpu.SemaphoreType.DMA((last - first,)),
        ],
        input_output_aliases={} if earlier is None else {3: 0},
        compiler_params=params(),
        cost_estimate=pl.CostEstimate(
            flops=2 * (last - first) * T * FW * DW,
            transcendentals=0,
            bytes_accessed=2 * (last - first) * FW * DW,
        ),
        name=f"grad_decoder_{begin}",
    )(*operands)


def grad_encoder_kernel(ranks_in, slots, turned_in, grad_out, bias_out, ranks, turned, dense, grad, rank_sem, turned_sem, sent):
    def load_ranks(layer):
        return pltpu.make_async_copy(ranks_in.at[layer], ranks.at[layer], rank_sem.at[layer])

    def load_turned(layer):
        return pltpu.make_async_copy(turned_in.at[layer], turned.at[layer], turned_sem.at[layer])

    def send(layer):
        return pltpu.make_async_copy(grad.at[layer], grad_out.at[layer], sent.at[layer])

    @pl.loop(0, LAYERS)
    def _(layer):
        load_ranks(layer).start()
        load_turned(layer).start()

    load_ranks(0).wait()
    unpack(ranks.at[0], slots.at[0], dense.at[0])
    for layer in range(LAYERS):
        load_turned(layer).wait()
        if layer + 1 < LAYERS:
            load_ranks(layer + 1).wait()
            unpack_next(ranks, slots, dense, layer + 1, 0, 1)
        grad[layer] = jnp.dot(turned[layer], dense[layer], preferred_element_type=F32).astype(BF)
        bias_out[layer : layer + 1, :] = jnp.dot(
            jnp.ones((16, T), BF), dense[layer], preferred_element_type=F32
        )[0:1]
        send(layer).start()

    each(LAYERS, send, "wait")


def grad_encoder_of(ranks, slots, turned):
    return pl.pallas_call(
        grad_encoder_kernel,
        in_specs=[ANY, HELD, ANY],
        out_specs=[ANY, HELD],
        out_shape=[
            jax.ShapeDtypeStruct((LAYERS, DW, FW), BF),
            jax.ShapeDtypeStruct((LAYERS, FW), F32),
        ],
        scratch_shapes=[
            pltpu.VMEM((LAYERS, T, FW), I32),
            pltpu.VMEM((LAYERS, DW, T), BF),
            pltpu.VMEM((LAYERS, T, FW), BF),
            pltpu.VMEM((LAYERS, DW, FW), BF),
            pltpu.SemaphoreType.DMA((LAYERS,)),
            pltpu.SemaphoreType.DMA((LAYERS,)),
            pltpu.SemaphoreType.DMA((LAYERS,)),
        ],
        compiler_params=params(),
        name="grad_encoder",
    )(ranks, slots, turned)


CHIPS = [[2 * chip + core for chip in range(8)] for core in range(2)]


def swap_cores(x):
    return lax.ppermute(x, "lat", [(i, i ^ 1) for i in range(16)])


def over_layer(x):
    return lax.all_to_all(x, "layer", 0, 0, tiled=True)


def over_chips(x):
    return lax.all_to_all(x, "lat", 0, 0, axis_index_groups=CHIPS, tiled=True)


def on_device(activations, targets, encoder, bias, decoder, active):
    lat = lax.axis_index("lat")
    first_row = ((lat % 2) * 8 + lat // 2) * 256
    active_t = jnp.swapaxes(active, 1, 2)
    columns, partial = encode(active_t, activations, encoder, bias)
    ranks, order = ranks_of(active_t, columns)
    settled = settle(over_layer(partial), order)
    settled, late = lax.optimization_barrier((settled, activations))
    turned = turn(late)
    latent, own, send = rebuild(ranks, over_layer(settled), decoder)
    half = (own + swap_cores(send).astype(F32)).astype(BF).reshape(8, 256, DW)
    total = jnp.sum(over_chips(half).astype(F32), axis=0)
    wanted = lax.dynamic_slice_in_dim(targets.reshape(LAYERS * T, DW), first_row, 256)
    error = (total - wanted.astype(F32)).astype(BF)
    mine = over_chips(jnp.broadcast_to(error[None], (8, 256, DW))).reshape(4, T, DW)
    other = swap_cores(mine)
    parts = over_layer(grad_act(columns, mine, other, decoder))
    grad_decoder = grad_decoder_part(latent, mine, other, 0, 3)
    parts, grad_decoder = lax.optimization_barrier((parts, grad_decoder))
    settled = over_layer(settle(parts, order))
    grad_decoder = grad_decoder_part(latent, mine, other, 3, LAYERS, grad_decoder)
    grad_encoder, grad_bias = grad_encoder_of(ranks, settled, turned)
    return (grad_encoder, grad_bias, grad_decoder)


def solution(mesh):
    placed = (
        P(None, None, "layer"),
        P(None, None, "layer"),
        P(None, "layer", "lat"),
        P(None, "lat"),
        P(None, "lat", "layer"),
        P(),
    )
    return jax.shard_map(
        on_device,
        mesh=mesh,
        in_specs=placed,
        out_specs=(P(None, "layer", "lat"), P(None, "lat"), P(None, "lat", "layer")),
        check_vma=False,
    )
```
